32 devices in a mesh: tm: 4 (over y, x), rows: 2 (over core), batch: 4 (over z).
Axes of the slice: x: 2, y: 2, z: 4, core: 2. Of those that a mesh axis runs over, the one named last changes fastest.
Arguments:
- inputs: bfloat16 [4, 8, 16, 128, 384], P('batch', 'tm', 'rows'), parts along dimension 0, may hold values from -16 to 16
- norm_gain: float32 [384], replicated, may hold values from 0.1 to 1.9
- norm_bias: float32 [384], replicated, may hold values from -3 to 3
- conv_weight: bfloat16 [3, 3, 3, 384, 384], replicated, may hold values from -0.0625 to 0.0625
- conv_bias: float32 [384], replicated, may hold values from -2 to 2
Outputs:
- decoded: bfloat16 [4, 8, 16, 128, 384], P('batch', 'tm', 'rows'), parts along dimension 0
The draws below stay inside these ranges and needn't reach their ends.
There are 4 independent parts, one for each index of `batch`. The reference program is written for one: setup_inputs(seed, part) draws one part's arguments, and reference() takes and returns one part's arrays. A program takes and returns all parts, laid end to end along the dimension named above; an argument that names none is the same for every part. Nothing has to cross between parts.
All inputs are finite; a program needn't handle non-finite values.
Results may differ from the reference program's by a relative error of at most 0.0025.
Values may be sent and summed in bfloat16 or wider, within the bound.
A program may use at most 128 MiB of HBM per device.

```python
import jax
import jax.numpy as jnp
from jax import lax

CHANNELS = 384
GROUPS = 32
WIDTH = 128
CLIPS = 1
FRAMES = 8
HEIGHT = 16


def draw_inputs(key, part):
    subkeys = jax.random.split(jax.random.fold_in(key, 17), 4)
    full_shape = (CLIPS, FRAMES, HEIGHT, WIDTH, CHANNELS)
    scales = 0.6 * jnp.exp(jax.random.uniform(subkeys[0], (CLIPS, FRAMES, HEIGHT, 1, 1), jnp.float32, -1.2, 1.2))
    offsets = 1.2 + 0.4 * jax.random.truncated_normal(subkeys[1], -5.0, 5.0, (CHANNELS,), jnp.float32)
    row_place = (jnp.arange(HEIGHT, dtype=jnp.float32) + 0.5) / HEIGHT
    row_ramp = (3.0 * row_place - 1.5).reshape(1, 1, HEIGHT, 1, 1)
    frame_level = jax.random.uniform(subkeys[3], (CLIPS, FRAMES, 1, 1, 1), jnp.float32, -1.2, 1.2)
    region = row_ramp + frame_level
    noisy_part = jax.random.truncated_normal(subkeys[2], -4.0, 4.0, full_shape, jnp.float32)
    values = noisy_part * scales + offsets + region
    return values.astype(jnp.bfloat16)


def bell_draw(key, extent, scale, limit, kind=jnp.bfloat16):
    values = jax.random.normal(key, extent, jnp.float32) * scale
    return jnp.minimum(jnp.maximum(values, -limit), limit).astype(kind)


def setup_inputs(seed: int = 0, part: int = 0) -> dict:
    key_list = jax.random.split(jax.random.key(seed), 6)
    own_keys = jax.random.split(jax.random.fold_in(key_list[5], part), 6)
    return {
        "inputs": draw_inputs(jax.random.fold_in(jax.random.fold_in(key_list[5], part), 71), part),
        "norm_gain": jnp.clip(1.0 + 0.18 * jax.random.normal(key_list[1], (CHANNELS,), jnp.float32), 0.1, 1.9),
        "norm_bias": bell_draw(key_list[2], (CHANNELS,), 0.5, 3.0, jnp.float32),
        "conv_weight": bell_draw(key_list[3], (3, 3, 3, CHANNELS, CHANNELS), (27 * CHANNELS) ** -0.5, 0.0625),
        "conv_bias": bell_draw(key_list[4], (CHANNELS,), 0.3, 2.0, jnp.float32),
    }


epsilon = 1e-06

def convolve(padded, conv_weight, frames, height, width):
    channels = padded.shape[-1]
    summed = jnp.zeros((padded.shape[0] * frames * height * width, conv_weight.shape[-1]), jnp.float32)
    for tap_time in range(3):
        for tap_row in range(3):
            slab_rows = padded[:, tap_time:tap_time + frames, tap_row:tap_row + height]
            columns = jnp.concatenate([slab_rows[:, :, :, 0:width], slab_rows[:, :, :, 1:width + 1], slab_rows[:, :, :, 2:width + 2]], axis=-1)
            kernel = conv_weight[tap_time, tap_row].reshape(3 * channels, -1)
            summed = summed + jnp.dot(columns.reshape(-1, 3 * channels), kernel, preferred_element_type=jnp.float32)
    return summed

def reference(inputs, norm_gain, norm_bias, conv_weight, conv_bias):
    values = inputs.astype(jnp.float32)
    channels = values.shape[-1]
    per_group = channels // GROUPS
    cell_count = 1.0 * CLIPS * FRAMES * HEIGHT * WIDTH * per_group
    chan_sum = lax.optimization_barrier(jnp.sum(values, axis=(0, 1, 2, 3)))
    group_mean = lax.optimization_barrier(jnp.sum(chan_sum.reshape(GROUPS, per_group), axis=1)) / cell_count
    centered = values - jnp.repeat(group_mean, per_group)
    chan_square = lax.optimization_barrier(jnp.sum(centered * centered, axis=(0, 1, 2, 3)))
    group_var = lax.optimization_barrier(jnp.sum(chan_square.reshape(GROUPS, per_group), axis=1)) / cell_count
    inverse = jnp.repeat(lax.rsqrt(group_var + epsilon), per_group)
    normed = centered * inverse * norm_gain + norm_bias
    active = (normed * jax.nn.sigmoid(normed)).astype(jnp.bfloat16)
    padded = jnp.pad(active, ((0, 0), (2, 0), (1, 1), (1, 1), (0, 0)))
    summed = convolve(padded, conv_weight, FRAMES, HEIGHT, WIDTH)
    result = values + summed.reshape(values.shape) + conv_bias
    return result.astype(jnp.bfloat16)
```

```python
import functools

import jax
import jax.numpy as jnp
from jax import lax
from jax.experimental import pallas as pl
from jax.experimental.pallas import tpu as pltpu
from jax.sharding import PartitionSpec as P

GROUPS = 32
MESH = pl.DeviceIdType.MESH
OWN_ROWS = 2

epsilon = 1e-06


def block_kernel(
    T, R, x_hbm, gain_ref, nbias_ref, w_hbm, cbias_ref, out_ref,
    xv, wv, hraw, eown, ehalo, own3, halo3, edge3, acc, stats,
    x_sem, w_sem, halo_send, halo_recv, eown_send, eown_recv,
    ehalo_send, ehalo_recv, stat_send, stat_recv,
):
    F, H, W, C = x_hbm.shape
    C3 = 3 * C
    n = T * R
    tm = lax.axis_index("tm")
    row = lax.axis_index("rows")
    me = tm * R + row

    def peer(offset):
        other = lax.rem(me + offset, n)
        return {"tm": other // R, "rows": lax.rem(other, R)}

    x_copies = [pltpu.make_async_copy(x_hbm.at[f], xv.at[f], x_sem.at[f]) for f in range(F)]
    w_copies = [
        pltpu.make_async_copy(
            w_hbm.at[kt, kh], wv.at[kt, :, pl.ds(kh * C, C)], w_sem.at[kt * 3 + kh]
        )
        for kt in range(3)
        for kh in range(3)
    ]
    barrier = pltpu.get_barrier_semaphore()
    for d in range(1, n):
        pl.semaphore_signal(barrier, inc=1, device_id=peer(d), device_id_type=MESH)
    for c in x_copies:
        c.start()
    pl.semaphore_wait(barrier, n - 1)

    def row_of(i):
        return jnp.where(i == 0, 0, jnp.where(i == 1, H - 1, i - 1))

    def halo_copy(i, r):
        return pltpu.make_async_remote_copy(
            src_ref=x_hbm.at[pl.ds(F - 2, 2), pl.ds(r, 1)],
            dst_ref=hraw.at[:, pl.ds(r, 1)],
            send_sem=halo_send.at[i],
            recv_sem=halo_recv.at[i],
            device_id={"tm": lax.rem(tm + 1, T), "rows": row},
            device_id_type=MESH,
        )

    def own_edge(side):
        r = H - 1 if side == 0 else 0
        target = row + 1 if side == 0 else row - 1
        return pltpu.make_async_remote_copy(
            src_ref=x_hbm.at[:, pl.ds(r, 1)],
            dst_ref=eown.at[side],
            send_sem=eown_send.at[side],
            recv_sem=eown_recv.at[side],
            device_id={"tm": tm, "rows": lax.rem(target + R, R)},
            device_id_type=MESH,
        )

    def halo_edge(side):
        r = H - 1 if side == 0 else 0
        target = row + 1 if side == 0 else row - 1
        return pltpu.make_async_remote_copy(
            src_ref=hraw.at[:, pl.ds(r, 1)],
            dst_ref=ehalo.at[side],
            send_sem=ehalo_send.at[side],
            recv_sem=ehalo_recv.at[side],
            device_id={"tm": tm, "rows": lax.rem(target + R, R)},
            device_id_type=MESH,
        )

    has_next, has_prev = tm < T - 1, tm > 0
    sends_edge = (row < R - 1, row > 0)
    gets_edge = (row > 0, row < R - 1)

    @pl.when(has_next)
    def _():
        for i in range(H):
            halo_copy(i, 0 if i == 0 else H - 1 if i == 1 else i - 1).start()

    for side in range(2):
        @pl.when(sends_edge[side])
        def _():
            own_edge(side).start()

    for c in w_copies:
        c.start()

    total = jnp.zeros((8, C), jnp.float32)
    square = jnp.zeros((8, C), jnp.float32)
    for f in range(F):
        x_copies[f].wait()

        def add_rows(r, carry):
            v = xv[f, r].astype(jnp.float32).reshape(W // 8, 8, C)
            return carry[0] + jnp.sum(v, axis=0), carry[1] + jnp.sum(v * v, axis=0)

        total, square = lax.fori_loop(0, H, add_rows, (total, square))
    stats[0, 0:8] = total
    stats[0, 8:16] = square

    def stat_copy(d):
        return pltpu.make_async_remote_copy(
            src_ref=stats.at[0],
            dst_ref=stats.at[d],
            send_sem=stat_send.at[d],
            recv_sem=stat_recv.at[d],
            device_id=peer(d),
            device_id_type=MESH,
        )

    for d in range(1, n):
        stat_copy(d).start()
    for f in range(F):
        def start_acc(r, _):
            acc[f, r + 1] = xv[f, r].astype(jnp.float32) + cbias_ref[...]
            return 0

        lax.fori_loop(0, H, start_acc, 0)
    for d in range(1, n):
        stat_copy(d).wait_recv()
    total = stats[0]
    for d in range(1, n):
        total = total + stats[d]
    sums = jnp.concatenate(
        [
            jnp.broadcast_to(jnp.sum(total[0:8], axis=0, keepdims=True), (8, C)),
            jnp.broadcast_to(jnp.sum(total[8:16], axis=0, keepdims=True), (8, C)),
        ],
        axis=0,
    )
    per_group = C // GROUPS
    channel = lax.broadcasted_iota(jnp.int32, (C, C), 0)
    other = lax.broadcasted_iota(jnp.int32, (C, C), 1)
    first = (other // per_group) * per_group
    member = jnp.where((channel >= first) & (channel < first + per_group), 1.0, 0.0)
    cells = 1.0 * F * H * W * per_group * n
    moments = (
        jnp.dot(
            sums,
            member.astype(jnp.float32),
            preferred_element_type=jnp.float32,
            precision=lax.Precision.HIGHEST,
        )
        / cells
    )
    mean = moments[0:1]
    var = jnp.maximum(moments[8:9] - mean * mean, 0.0)
    half_scale = lax.rsqrt(var + epsilon) * gain_ref[...] * 0.5
    half_bias = nbias_ref[...] * 0.5

    column = lax.broadcasted_iota(jnp.int32, (W, C), 0)

    def activate(raw, put):
        h = (raw.astype(jnp.float32) - mean) * half_scale + half_bias
        a = h + h * jnp.tanh(h)
        put(0, jnp.where(column == 0, 0.0, pltpu.roll(a, 1, 0)).astype(jnp.bfloat16))
        put(1, a.astype(jnp.bfloat16))
        put(2, jnp.where(column == W - 1, 0.0, pltpu.roll(a, W - 1, 0)).astype(jnp.bfloat16))

    for f in range(F):
        def own_row(r, _):
            def put(k, v):
                own3[f, r, :, k * C : (k + 1) * C] = v

            activate(xv[f, r], put)
            return 0

        lax.fori_loop(0, H, own_row, 0)

    @pl.when(has_prev)
    def _():
        for i in range(2):
            halo_copy(i, 0 if i == 0 else H - 1).wait_recv()
        for side in range(2):
            @pl.when(sends_edge[side])
            def _():
                halo_edge(side).start()

    for c in w_copies:
        c.wait()

    def product(lhs, kt, lo=0, hi=3):
        return jnp.dot(
            lhs, wv[kt, :, lo * C : hi * C], preferred_element_type=jnp.float32
        )

    def own_rows(g, _):
        r0 = g * OWN_ROWS
        for kt in range(3):
            count = F - 2 + kt
            if count <= 0:
                continue
            lhs = own3[0:count, pl.ds(r0, OWN_ROWS)].reshape(count * OWN_ROWS * W, C3)
            y = product(lhs, kt)
            for kh in range(3):
                part = y[:, kh * C : (kh + 1) * C].reshape(count, OWN_ROWS, W, C)
                acc[2 - kt : 2 - kt + count, pl.ds(r0 + 2 - kh, OWN_ROWS)] += part
        return 0

    lax.fori_loop(0, H // OWN_ROWS, own_rows, 0)

    for side in range(2):
        kh = 0 if side == 0 else 2
        at = 1 if side == 0 else H

        @pl.when(gets_edge[side])
        def _():
            own_edge(side).wait_recv()
            for f in range(F):
                def put(k, v):
                    edge3[f, :, k * C : (k + 1) * C] = v

                activate(eown[side, f, 0], put)
            for kt in range(3):
                count = F - 2 + kt
                if count > 0:
                    lhs = edge3[0:count].reshape(count * W, C3)
                    acc[2 - kt : 2 - kt + count, at] += product(lhs, kt, kh, kh + 1).reshape(
                        count, W, C
                    )

    @pl.when(has_prev)
    def _():
        def halo_row(i, _):
            r = row_of(i)

            @pl.when(i >= 2)
            def _():
                halo_copy(i, r).wait_recv()

            for f in range(2):
                def put(k, v):
                    halo3[f, :, k * C : (k + 1) * C] = v

                activate(hraw[f, r], put)
            y = product(halo3[...].reshape(2 * W, C3), 0)
            z = product(halo3[1], 1)
            for kh in range(3):
                cols = slice(kh * C, (kh + 1) * C)
                acc[0, r + 2 - kh] += y[:W, cols] + z[:, cols]
                acc[1, r + 2 - kh] += y[W:, cols]
            return 0

        lax.fori_loop(0, 2, halo_row, 0)
        for side in range(2):
            kh = 0 if side == 0 else 2
            at = 1 if side == 0 else H

            @pl.when(gets_edge[side])
            def _():
                halo_edge(side).wait_recv()
                for f in range(2):
                    def put(k, v):
                        halo3[f, :, k * C : (k + 1) * C] = v

                    activate(ehalo[side, f, 0], put)
                y = product(halo3[...].reshape(2 * W, C3), 0, kh, kh + 1)
                z = product(halo3[1], 1, kh, kh + 1)
                acc[0, at] += y[:W] + z
                acc[1, at] += y[W:]

        lax.fori_loop(2, H, halo_row, 0)

    for f in range(F):
        def finish(r, _):
            out_ref[f, r] = acc[f, r + 1].astype(out_ref.dtype)
            return 0

        lax.fori_loop(0, H, finish, 0)

    for d in range(1, n):
        stat_copy(d).wait_send()

    @pl.when(has_next)
    def _():
        for i in range(H):
            halo_copy(i, 0 if i == 0 else H - 1 if i == 1 else i - 1).wait_send()

    for side in range(2):
        @pl.when(sends_edge[side])
        def _():
            own_edge(side).wait_send()

            @pl.when(has_prev)
            def _():
                halo_edge(side).wait_send()


def shards(T, R, inputs, norm_gain, norm_bias, conv_weight, conv_bias):
    _, F, H, W, C = inputs.shape
    n = T * R
    vmem = pl.BlockSpec(memory_space=pltpu.VMEM)
    anywhere = pl.BlockSpec(memory_space=pl.ANY)
    dma = pltpu.SemaphoreType.DMA
    out = pl.pallas_call(
        functools.partial(block_kernel, T, R),
        out_shape=jax.ShapeDtypeStruct((F, H, W, C), inputs.dtype),
        in_specs=[anywhere, vmem, vmem, anywhere, vmem],
        out_specs=vmem,
        scratch_shapes=[
            pltpu.VMEM((F, H, W, C), jnp.bfloat16),
            pltpu.VMEM((3, 3 * C, 3 * C), jnp.bfloat16),
            pltpu.VMEM((2, H, W, C), jnp.bfloat16),
            pltpu.VMEM((2, F, 1, W, C), jnp.bfloat16),
            pltpu.VMEM((2, 2, 1, W, C), jnp.bfloat16),
            pltpu.VMEM((F, H, W, 3 * C), jnp.bfloat16),
            pltpu.VMEM((2, W, 3 * C), jnp.bfloat16),
            pltpu.VMEM((F, W, 3 * C), jnp.bfloat16),
            pltpu.VMEM((F, H + 2, W, C), jnp.float32),
            pltpu.VMEM((n, 16, C), jnp.float32),
            dma((F,)),
            dma((9,)),
            dma((H,)),
            dma((H,)),
            dma((2,)),
            dma((2,)),
            dma((2,)),
            dma((2,)),
            dma((n,)),
            dma((n,)),
        ],
        compiler_params=pltpu.CompilerParams(
            collective_id=0, has_side_effects=True, vmem_limit_bytes=50 * 1024 * 1024
        ),
        name="norm_conv_block",
    )(
        inputs.reshape(F, H, W, C),
        norm_gain.reshape(1, C),
        norm_bias.reshape(1, C),
        conv_weight.reshape(3, 3, 3 * C, C),
        conv_bias.reshape(1, C),
    )
    return out.reshape(inputs.shape)


def solution(mesh):
    placed = (P("batch", "tm", "rows", None, None), P(), P(), P(), P())
    return jax.shard_map(
        functools.partial(shards, mesh.shape["tm"], mesh.shape["rows"]),
        mesh=mesh,
        in_specs=placed,
        out_specs=P("batch", "tm", "rows", None, None),
        check_vma=False,
    )
```

```python
import functools

import jax
import jax.numpy as jnp
from jax import lax
from jax.experimental import pallas as pl
from jax.experimental.pallas import tpu as pltpu
from jax.sharding import PartitionSpec as P

GROUPS = 32
MESH = pl.DeviceIdType.MESH
OWN_ROWS = 2
EARLY = 1

epsilon = 1e-06


def block_kernel(
    T, R, x_hbm, gain_hbm, nbias_hbm, w_hbm, cbias_hbm, out_ref,
    params, p_sem, xv, wv, hraw, eown, ehalo, own3, halo3, edge3, acc, stats,
    x_sem, w_sem, halo_send, halo_recv, eown_send, eown_recv,
    ehalo_send, ehalo_recv, stat_send, stat_recv,
):
    F, H, W, C = x_hbm.shape
    C3 = 3 * C
    n = T * R
    tm = lax.axis_index("tm")
    row = lax.axis_index("rows")
    me = tm * R + row

    def peer(offset):
        other = lax.rem(me + offset, n)
        return {"tm": other // R, "rows": lax.rem(other, R)}

    x_copies = [pltpu.make_async_copy(x_hbm.at[f], xv.at[f], x_sem.at[f]) for f in range(F)]
    w_copies = [
        pltpu.make_async_copy(
            w_hbm.at[kt, kh], wv.at[kt, :, pl.ds(kh * C, C)], w_sem.at[kt * 3 + kh]
        )
        for kt in range(3)
        for kh in range(3)
    ]
    p_copies = [
        pltpu.make_async_copy(p, params.at[k, 0], p_sem.at[k])
        for k, p in enumerate((gain_hbm, nbias_hbm, cbias_hbm))
    ]
    barrier = pltpu.get_barrier_semaphore()
    for d in range(1, n):
        pl.semaphore_signal(barrier, inc=1, device_id=peer(d), device_id_type=MESH)
    for c in x_copies + p_copies:
        c.start()
    pl.semaphore_wait(barrier, n - 1)

    def row_of(i):
        return jnp.where(i == 0, 0, jnp.where(i == 1, H - 1, i - 1))

    def halo_copy(i, r):
        return pltpu.make_async_remote_copy(
            src_ref=x_hbm.at[pl.ds(F - 2, 2), pl.ds(r, 1)],
            dst_ref=hraw.at[:, pl.ds(r, 1)],
            send_sem=halo_send.at[i],
            recv_sem=halo_recv.at[i],
            device_id={"tm": lax.rem(tm + 1, T), "rows": row},
            device_id_type=MESH,
        )

    def own_edge(side):
        r = H - 1 if side == 0 else 0
        target = row + 1 if side == 0 else row - 1
        return pltpu.make_async_remote_copy(
            src_ref=x_hbm.at[:, pl.ds(r, 1)],
            dst_ref=eown.at[side],
            send_sem=eown_send.at[side],
            recv_sem=eown_recv.at[side],
            device_id={"tm": tm, "rows": lax.rem(target + R, R)},
            device_id_type=MESH,
        )

    def halo_edge(side):
        r = H - 1 if side == 0 else 0
        target = row + 1 if side == 0 else row - 1
        return pltpu.make_async_remote_copy(
            src_ref=hraw.at[:, pl.ds(r, 1)],
            dst_ref=ehalo.at[side],
            send_sem=ehalo_send.at[side],
            recv_sem=ehalo_recv.at[side],
            device_id={"tm": tm, "rows": lax.rem(target + R, R)},
            device_id_type=MESH,
        )

    has_next, has_prev = tm < T - 1, tm > 0
    sends_edge = (row < R - 1, row > 0)
    gets_edge = (row > 0, row < R - 1)

    @pl.when(has_next)
    def _():
        for i in range(EARLY):
            halo_copy(i, 0 if i == 0 else H - 1 if i == 1 else i - 1).start()

    for side in range(2):
        @pl.when(sends_edge[side])
        def _():
            own_edge(side).start()

    for c in w_copies:
        c.start()

    total = jnp.zeros((8, C), jnp.float32)
    square = jnp.zeros((8, C), jnp.float32)
    for f in range(F):
        x_copies[f].wait()

        def add_rows(r, carry):
            v = xv[f, r].astype(jnp.float32).reshape(W // 8, 8, C)
            return carry[0] + jnp.sum(v, axis=0), carry[1] + jnp.sum(v * v, axis=0)

        total, square = lax.fori_loop(0, H, add_rows, (total, square))
    stats[0, 0:8] = total
    stats[0, 8:16] = square

    def stat_copy(d):
        return pltpu.make_async_remote_copy(
            src_ref=stats.at[0],
            dst_ref=stats.at[d],
            send_sem=stat_send.at[d],
            recv_sem=stat_recv.at[d],
            device_id=peer(d),
            device_id_type=MESH,
        )

    for d in range(1, n):
        stat_copy(d).start()

    @pl.when(has_next)
    def _():
        for i in range(EARLY, H):
            halo_copy(i, 0 if i == 0 else H - 1 if i == 1 else i - 1).start()

    for c in p_copies:
        c.wait()
    for f in range(F):
        def start_acc(r, _):
            acc[f, r + 1] = xv[f, r].astype(jnp.float32) + params[2]
            return 0

        lax.fori_loop(0, H, start_acc, 0)
    for d in range(1, n):
        stat_copy(d).wait_recv()
    total = stats[0]
    for d in range(1, n):
        total = total + stats[d]
    sums = jnp.concatenate(
        [
            jnp.broadcast_to(jnp.sum(total[0:8], axis=0, keepdims=True), (8, C)),
            jnp.broadcast_to(jnp.sum(total[8:16], axis=0, keepdims=True), (8, C)),
        ],
        axis=0,
    )
    per_group = C // GROUPS
    channel = lax.broadcasted_iota(jnp.int32, (C, C), 0)
    other = lax.broadcasted_iota(jnp.int32, (C, C), 1)
    first = (other // per_group) * per_group
    member = jnp.where((channel >= first) & (channel < first + per_group), 1.0, 0.0)
    cells = 1.0 * F * H * W * per_group * n
    moments = (
        jnp.dot(
            sums,
            member.astype(jnp.float32),
            preferred_element_type=jnp.float32,
            precision=lax.Precision.HIGHEST,
        )
        / cells
    )
    mean = moments[0:1]
    var = jnp.maximum(moments[8:9] - mean * mean, 0.0)
    half_scale = lax.rsqrt(var + epsilon) * params[0] * 0.5
    half_bias = params[1] * 0.5

    column = lax.broadcasted_iota(jnp.int32, (W, C), 0)

    def activate(raw, put):
        h = (raw.astype(jnp.float32) - mean) * half_scale + half_bias
        a = h + h * jnp.tanh(h)
        put(0, jnp.where(column == 0, 0.0, pltpu.roll(a, 1, 0)).astype(jnp.bfloat16))
        put(1, a.astype(jnp.bfloat16))
        put(2, jnp.where(column == W - 1, 0.0, pltpu.roll(a, W - 1, 0)).astype(jnp.bfloat16))

    for f in range(F):
        def own_row(r, _):
            def put(k, v):
                own3[f, r, :, k * C : (k + 1) * C] = v

            activate(xv[f, r], put)
            return 0

        lax.fori_loop(0, H, own_row, 0)

    @pl.when(has_prev)
    def _():
        for i in range(2):
            halo_copy(i, 0 if i == 0 else H - 1).wait_recv()
        for side in range(2):
            @pl.when(sends_edge[side])
            def _():
                halo_edge(side).start()

    for c in w_copies:
        c.wait()

    def product(lhs, kt, lo=0, hi=3):
        return jnp.dot(
            lhs, wv[kt, :, lo * C : hi * C], preferred_element_type=jnp.float32
        )

    def finish(r, _):
        for f in range(F):
            out_ref[f, r] = acc[f, r + 1].astype(out_ref.dtype)
        return 0

    def own_rows(g, _):
        r0 = g * OWN_ROWS
        for kt in range(3):
            count = F - 2 + kt
            if count <= 0:
                continue
            lhs = own3[0:count, pl.ds(r0, OWN_ROWS)].reshape(count * OWN_ROWS * W, C3)
            y = product(lhs, kt)
            for kh in range(3):
                part = y[:, kh * C : (kh + 1) * C].reshape(count, OWN_ROWS, W, C)
                acc[2 - kt : 2 - kt + count, pl.ds(r0 + 2 - kh, OWN_ROWS)] += part
        return 0

    lax.fori_loop(0, H // OWN_ROWS, own_rows, 0)

    for side in range(2):
        kh = 0 if side == 0 else 2
        at = 1 if side == 0 else H

        @pl.when(gets_edge[side])
        def _():
            own_edge(side).wait_recv()
            for f in range(F):
                def put(k, v):
                    edge3[f, :, k * C : (k + 1) * C] = v

                activate(eown[side, f, 0], put)
            for kt in range(3):
                count = F - 2 + kt
                if count > 0:
                    lhs = edge3[0:count].reshape(count * W, C3)
                    acc[2 - kt : 2 - kt + count, at] += product(lhs, kt, kh, kh + 1).reshape(
                        count, W, C
                    )

    @pl.when(has_prev)
    def _():
        def halo_row(i, _):
            r = row_of(i)

            @pl.when(i >= 2)
            def _():
                halo_copy(i, r).wait_recv()

            for f in range(2):
                def put(k, v):
                    halo3[f, :, k * C : (k + 1) * C] = v

                activate(hraw[f, r], put)
            y = product(halo3[...].reshape(2 * W, C3), 0)
            z = product(halo3[1], 1)
            for kh in range(3):
                cols = slice(kh * C, (kh + 1) * C)
                acc[0, r + 2 - kh] += y[:W, cols] + z[:, cols]
                acc[1, r + 2 - kh] += y[W:, cols]

            @pl.when(i >= 2)
            def _():
                finish(i - 2, 0)

            return 0

        lax.fori_loop(0, 2, halo_row, 0)
        for side in range(2):
            kh = 0 if side == 0 else 2
            at = 1 if side == 0 else H

            @pl.when(gets_edge[side])
            def _():
                halo_edge(side).wait_recv()
                for f in range(2):
                    def put(k, v):
                        halo3[f, :, k * C : (k + 1) * C] = v

                    activate(ehalo[side, f, 0], put)
                y = product(halo3[...].reshape(2 * W, C3), 0, kh, kh + 1)
                z = product(halo3[1], 1, kh, kh + 1)
                acc[0, at] += y[:W] + z
                acc[1, at] += y[W:]

        lax.fori_loop(2, H, halo_row, 0)
        lax.fori_loop(max(H - 2, 0), H, finish, 0)

    @pl.when(jnp.logical_not(has_prev))
    def _():
        lax.fori_loop(0, H, finish, 0)

    for d in range(1, n):
        stat_copy(d).wait_send()

    @pl.when(has_next)
    def _():
        for i in range(H):
            halo_copy(i, 0 if i == 0 else H - 1 if i == 1 else i - 1).wait_send()

    for side in range(2):
        @pl.when(sends_edge[side])
        def _():
            own_edge(side).wait_send()

            @pl.when(has_prev)
            def _():
                halo_edge(side).wait_send()


def shards(T, R, inputs, norm_gain, norm_bias, conv_weight, conv_bias):
    _, F, H, W, C = inputs.shape
    n = T * R
    vmem = pl.BlockSpec(memory_space=pltpu.VMEM)
    hbm = pl.BlockSpec(memory_space=pltpu.HBM)
    anywhere = pl.BlockSpec(memory_space=pl.ANY)
    dma = pltpu.SemaphoreType.DMA
    out = pl.pallas_call(
        functools.partial(block_kernel, T, R),
        out_shape=jax.ShapeDtypeStruct((F, H, W, C), inputs.dtype),
        in_specs=[hbm, anywhere, anywhere, hbm, anywhere],
        out_specs=vmem,
        scratch_shapes=[
            pltpu.VMEM((3, 1, C), jnp.float32),
            dma((3,)),
            pltpu.VMEM((F, H, W, C), jnp.bfloat16),
            pltpu.VMEM((3, 3 * C, 3 * C), jnp.bfloat16),
            pltpu.VMEM((2, H, W, C), jnp.bfloat16),
            pltpu.VMEM((2, F, 1, W, C), jnp.bfloat16),
            pltpu.VMEM((2, 2, 1, W, C), jnp.bfloat16),
            pltpu.VMEM((F, H, W, 3 * C), jnp.bfloat16),
            pltpu.VMEM((2, W, 3 * C), jnp.bfloat16),
            pltpu.VMEM((F, W, 3 * C), jnp.bfloat16),
            pltpu.VMEM((F, H + 2, W, C), jnp.float32),
            pltpu.VMEM((n, 16, C), jnp.float32),
            dma((F,)),
            dma((9,)),
            dma((H,)),
            dma((H,)),
            dma((2,)),
            dma((2,)),
            dma((2,)),
            dma((2,)),
            dma((n,)),
            dma((n,)),
        ],
        compiler_params=pltpu.CompilerParams(
            collective_id=0, has_side_effects=True, vmem_limit_bytes=50 * 1024 * 1024
        ),
        name="norm_conv_block",
    )(
        inputs.reshape(F, H, W, C),
        norm_gain,
        norm_bias,
        conv_weight.reshape(3, 3, 3 * C, C),
        conv_bias,
    )
    return out.reshape(inputs.shape)


def solution(mesh):
    placed = (P("batch", "tm", "rows", None, None), P(), P(), P(), P())
    return jax.shard_map(
        functools.partial(shards, mesh.shape["tm"], mesh.shape["rows"]),
        mesh=mesh,
        in_specs=placed,
        out_specs=P("batch", "tm", "rows", None, None),
        check_vma=False,
    )
```

```python
import functools

import jax
import jax.numpy as jnp
from jax import lax
from jax.experimental import pallas as pl
from jax.experimental.pallas import tpu as pltpu
from jax.sharding import PartitionSpec as P

GROUPS = 32
MESH = pl.DeviceIdType.MESH
OWN_ROWS = 2
EARLY = 1

epsilon = 1e-06


def block_kernel(
    T, R, x_hbm, gain_hbm, nbias_hbm, w_hbm, cbias_hbm, out_ref,
    params, p_sem, xv, wv, hraw, eown, ehalo, own3, halo3, edge3, acc, stats,
    x_sem, w_sem, halo_send, halo_recv, eown_send, eown_recv,
    ehalo_send, ehalo_recv, stat_send, stat_recv,
):
    F, H, W, C = x_hbm.shape
    C3 = 3 * C
    n = T * R
    tm = lax.axis_index("tm")
    row = lax.axis_index("rows")
    me = tm * R + row

    def peer(offset):
        other = lax.rem(me + offset, n)
        return {"tm": other // R, "rows": lax.rem(other, R)}

    x_copies = [pltpu.make_async_copy(x_hbm.at[f], xv.at[f], x_sem.at[f]) for f in range(F)]
    w_copies = [
        pltpu.make_async_copy(
            w_hbm.at[kt, kh], wv.at[kt, :, pl.ds(kh * C, C)], w_sem.at[kt * 3 + kh]
        )
        for kt in range(3)
        for kh in range(3)
    ]
    p_copies = [
        pltpu.make_async_copy(p, params.at[k, 0], p_sem.at[k])
        for k, p in enumerate((gain_hbm, nbias_hbm, cbias_hbm))
    ]
    barrier = pltpu.get_barrier_semaphore()
    for d in range(1, n):
        pl.semaphore_signal(barrier, inc=1, device_id=peer(d), device_id_type=MESH)
    for c in x_copies + p_copies:
        c.start()
    pl.semaphore_wait(barrier, n - 1)

    def row_of(i):
        return jnp.where(i == 0, 0, jnp.where(i == 1, H - 1, i - 1))

    def halo_copy(i, r):
        return pltpu.make_async_remote_copy(
            src_ref=x_hbm.at[pl.ds(F - 2, 2), pl.ds(r, 1)],
            dst_ref=hraw.at[:, pl.ds(r, 1)],
            send_sem=halo_send.at[i],
            recv_sem=halo_recv.at[i],
            device_id={"tm": lax.rem(tm + 1, T), "rows": row},
            device_id_type=MESH,
        )

    def own_edge(side):
        r = H - 1 if side == 0 else 0
        target = row + 1 if side == 0 else row - 1
        return pltpu.make_async_remote_copy(
            src_ref=x_hbm.at[:, pl.ds(r, 1)],
            dst_ref=eown.at[side],
            send_sem=eown_send.at[side],
            recv_sem=eown_recv.at[side],
            device_id={"tm": tm, "rows": lax.rem(target + R, R)},
            device_id_type=MESH,
        )

    def halo_edge(side):
        r = H - 1 if side == 0 else 0
        target = row + 1 if side == 0 else row - 1
        return pltpu.make_async_remote_copy(
            src_ref=hraw.at[:, pl.ds(r, 1)],
            dst_ref=ehalo.at[side],
            send_sem=ehalo_send.at[side],
            recv_sem=ehalo_recv.at[side],
            device_id={"tm": tm, "rows": lax.rem(target + R, R)},
            device_id_type=MESH,
        )

    has_next, has_prev = tm < T - 1, tm > 0
    sends_edge = (row < R - 1, row > 0)
    gets_edge = (row > 0, row < R - 1)

    @pl.when(has_next)
    def _():
        for i in range(EARLY):
            halo_copy(i, 0 if i == 0 else H - 1 if i == 1 else i - 1).start()

    for side in range(2):
        @pl.when(sends_edge[side])
        def _():
            own_edge(side).start()

    for c in w_copies:
        c.start()

    total = jnp.zeros((8, C), jnp.float32)
    square = jnp.zeros((8, C), jnp.float32)
    for f in range(F):
        x_copies[f].wait()

        def add_rows(r, carry):
            v = xv[f, r].astype(jnp.float32).reshape(W // 8, 8, C)
            return carry[0] + jnp.sum(v, axis=0), carry[1] + jnp.sum(v * v, axis=0)

        total, square = lax.fori_loop(0, H, add_rows, (total, square))
    stats[0, 0:8] = total
    stats[0, 8:16] = square

    def stat_copy(d):
        return pltpu.make_async_remote_copy(
            src_ref=stats.at[0],
            dst_ref=stats.at[d],
            send_sem=stat_send.at[d],
            recv_sem=stat_recv.at[d],
            device_id=peer(d),
            device_id_type=MESH,
        )

    for d in range(1, n):
        stat_copy(d).start()

    @pl.when(has_next)
    def _():
        for i in range(EARLY, H):
            halo_copy(i, 0 if i == 0 else H - 1 if i == 1 else i - 1).start()

    for c in p_copies:
        c.wait()
    for f in range(F):
        def start_acc(r, _):
            acc[f, r + 1] = xv[f, r].astype(jnp.float32) + params[2]
            return 0

        lax.fori_loop(0, H, start_acc, 0)
    for d in range(1, n):
        stat_copy(d).wait_recv()
    total = stats[0]
    for d in range(1, n):
        total = total + stats[d]
    sums = jnp.concatenate(
        [
            jnp.broadcast_to(jnp.sum(total[0:8], axis=0, keepdims=True), (8, C)),
            jnp.broadcast_to(jnp.sum(total[8:16], axis=0, keepdims=True), (8, C)),
        ],
        axis=0,
    )
    per_group = C // GROUPS
    channel = lax.broadcasted_iota(jnp.int32, (C, C), 0)
    other = lax.broadcasted_iota(jnp.int32, (C, C), 1)
    first = (other // per_group) * per_group
    member = jnp.where((channel >= first) & (channel < first + per_group), 1.0, 0.0)
    cells = 1.0 * F * H * W * per_group * n
    moments = (
        jnp.dot(
            sums,
            member.astype(jnp.float32),
            preferred_element_type=jnp.float32,
            precision=lax.Precision.HIGHEST,
        )
        / cells
    )
    mean = moments[0:1]
    var = jnp.maximum(moments[8:9] - mean * mean, 0.0)
    half_scale = lax.rsqrt(var + epsilon) * params[0] * 0.5
    half_bias = params[1] * 0.5

    column = lax.broadcasted_iota(jnp.int32, (W, C), 0)

    def activate(raw, put):
        h = (raw.astype(jnp.float32) - mean) * half_scale + half_bias
        a = h + h * jnp.tanh(h)
        put(0, jnp.where(column == 0, 0.0, pltpu.roll(a, 1, 0)).astype(jnp.bfloat16))
        put(1, a.astype(jnp.bfloat16))
        put(2, jnp.where(column == W - 1, 0.0, pltpu.roll(a, W - 1, 0)).astype(jnp.bfloat16))

    for f in range(F):
        def own_row(r, _):
            def put(k, v):
                own3[f, r, :, k * C : (k + 1) * C] = v

            activate(xv[f, r], put)
            return 0

        lax.fori_loop(0, H, own_row, 0)

    @pl.when(has_prev)
    def _():
        for i in range(2):
            halo_copy(i, 0 if i == 0 else H - 1).wait_recv()
        for side in range(2):
            @pl.when(sends_edge[side])
            def _():
                halo_edge(side).start()

    for c in w_copies:
        c.wait()

    def product(lhs, kt, lo=0, hi=3):
        return jnp.dot(
            lhs, wv[kt, :, lo * C : hi * C], preferred_element_type=jnp.float32
        )

    def finish(r, _):
        for f in range(F):
            out_ref[f, r] = acc[f, r + 1].astype(out_ref.dtype)
        return 0

    def own_rows(g, _):
        r0 = g * OWN_ROWS
        for kt in range(3):
            count = F - 2 + kt
            if count <= 0:
                continue
            lhs = own3[0:count, pl.ds(r0, OWN_ROWS)].reshape(count * OWN_ROWS * W, C3)
            y = product(lhs, kt)
            for kh in range(3):
                part = y[:, kh * C : (kh + 1) * C].reshape(count, OWN_ROWS, W, C)
                acc[2 - kt : 2 - kt + count, pl.ds(r0 + 2 - kh, OWN_ROWS)] += part
        return 0

    lax.fori_loop(0, H // OWN_ROWS, own_rows, 0)

    for side in range(2):
        kh = 0 if side == 0 else 2
        at = 1 if side == 0 else H

        @pl.when(gets_edge[side])
        def _():
            own_edge(side).wait_recv()
            for f in range(F):
                def put(k, v):
                    edge3[f, :, k * C : (k + 1) * C] = v

                activate(eown[side, f, 0], put)
            for kt in range(3):
                count = F - 2 + kt
                if count > 0:
                    lhs = edge3[0:count].reshape(count * W, C3)
                    acc[2 - kt : 2 - kt + count, at] += product(lhs, kt, kh, kh + 1).reshape(
                        count, W, C
                    )

    @pl.when(has_prev)
    def _():
        def halo_row(i, _):
            r = row_of(i)

            @pl.when(i >= 2)
            def _():
                halo_copy(i, r).wait_recv()

            for f in range(2):
                def put(k, v):
                    halo3[f, :, k * C : (k + 1) * C] = v

                activate(hraw[f, r], put)
            y = product(halo3[...].reshape(2 * W, C3), 0)
            z = product(halo3[1], 1)
            for kh in range(3):
                cols = slice(kh * C, (kh + 1) * C)
                acc[0, r + 2 - kh] += y[:W, cols] + z[:, cols]
                acc[1, r + 2 - kh] += y[W:, cols]

            @pl.when(i >= 2)
            def _():
                finish(i - 2, 0)

            return 0

        lax.fori_loop(0, 2, halo_row, 0)
        for side in range(2):
            kh = 0 if side == 0 else 2
            at = 1 if side == 0 else H

            @pl.when(gets_edge[side])
            def _():
                halo_edge(side).wait_recv()
                for f in range(2):
                    def put(k, v):
                        halo3[f, :, k * C : (k + 1) * C] = v

                    activate(ehalo[side, f, 0], put)
                y = product(halo3[...].reshape(2 * W, C3), 0, kh, kh + 1)
                z = product(halo3[1], 1, kh, kh + 1)
                acc[0, at] += y[:W] + z
                acc[1, at] += y[W:]

        lax.fori_loop(2, H, halo_row, 0)
        lax.fori_loop(max(H - 2, 0), H, finish, 0)

    @pl.when(jnp.logical_not(has_prev))
    def _():
        lax.fori_loop(0, H, finish, 0)

    for d in range(1, n):
        stat_copy(d).wait_send()

    @pl.when(has_next)
    def _():
        for i in range(H):
            halo_copy(i, 0 if i == 0 else H - 1 if i == 1 else i - 1).wait_send()

    for side in range(2):
        @pl.when(sends_edge[side])
        def _():
            own_edge(side).wait_send()

            @pl.when(has_prev)
            def _():
                halo_edge(side).wait_send()


def shards(T, R, inputs, norm_gain, norm_bias, conv_weight, conv_bias):
    _, F, H, W, C = inputs.shape
    n = T * R

    def pin(a):
        return pltpu.with_memory_space_constraint(a, pltpu.HBM)

    vmem = pl.BlockSpec(memory_space=pltpu.VMEM)
    hbm = pl.BlockSpec(memory_space=pltpu.HBM)
    anywhere = pl.BlockSpec(memory_space=pl.ANY)
    dma = pltpu.SemaphoreType.DMA
    out = pl.pallas_call(
        functools.partial(block_kernel, T, R),
        out_shape=jax.ShapeDtypeStruct((F, H, W, C), inputs.dtype),
        in_specs=[hbm, anywhere, anywhere, hbm, anywhere],
        out_specs=vmem,
        scratch_shapes=[
            pltpu.VMEM((3, 1, C), jnp.float32),
            dma((3,)),
            pltpu.VMEM((F, H, W, C), jnp.bfloat16),
            pltpu.VMEM((3, 3 * C, 3 * C), jnp.bfloat16),
            pltpu.VMEM((2, H, W, C), jnp.bfloat16),
            pltpu.VMEM((2, F, 1, W, C), jnp.bfloat16),
            pltpu.VMEM((2, 2, 1, W, C), jnp.bfloat16),
            pltpu.VMEM((F, H, W, 3 * C), jnp.bfloat16),
            pltpu.VMEM((2, W, 3 * C), jnp.bfloat16),
            pltpu.VMEM((F, W, 3 * C), jnp.bfloat16),
            pltpu.VMEM((F, H + 2, W, C), jnp.float32),
            pltpu.VMEM((n, 16, C), jnp.float32),
            dma((F,)),
            dma((9,)),
            dma((H,)),
            dma((H,)),
            dma((2,)),
            dma((2,)),
            dma((2,)),
            dma((2,)),
            dma((n,)),
            dma((n,)),
        ],
        compiler_params=pltpu.CompilerParams(
            collective_id=0, has_side_effects=True, vmem_limit_bytes=50 * 1024 * 1024
        ),
        name="norm_conv_block",
    )(
        pin(inputs.reshape(F, H, W, C)),
        pin(norm_gain),
        pin(norm_bias),
        pin(conv_weight.reshape(3, 3, 3 * C, C)),
        pin(conv_bias),
    )
    return out.reshape(inputs.shape)


def solution(mesh):
    placed = (P("batch", "tm", "rows", None, None), P(), P(), P(), P())
    return jax.shard_map(
        functools.partial(shards, mesh.shape["tm"], mesh.shape["rows"]),
        mesh=mesh,
        in_specs=placed,
        out_specs=P("batch", "tm", "rows", None, None),
        check_vma=False,
    )
```

```python
import functools

import jax
import jax.numpy as jnp
from jax import lax
from jax.experimental import pallas as pl
from jax.experimental.pallas import tpu as pltpu
from jax.sharding import PartitionSpec as P

GROUPS = 32
MESH = pl.DeviceIdType.MESH
OWN_ROWS = 4
EARLY = 2

epsilon = 1e-06


def block_kernel(
    T, R, x_hbm, gain_hbm, nbias_hbm, w_hbm, cbias_hbm, out_ref,
    params, p_sem, xv, wv, hraw, eown, ehalo, own3, halo3, edge3, acc, stats,
    x_sem, w_sem, halo_send, halo_recv, eown_send, eown_recv,
    ehalo_send, ehalo_recv, stat_send, stat_recv,
):
    F, H, W, C = x_hbm.shape
    C3 = 3 * C
    n = T * R
    tm = lax.axis_index("tm")
    row = lax.axis_index("rows")
    me = tm * R + row

    def peer(offset):
        other = lax.rem(me + offset, n)
        return {"tm": other // R, "rows": lax.rem(other, R)}

    x_copies = [pltpu.make_async_copy(x_hbm.at[f], xv.at[f], x_sem.at[f]) for f in range(F)]
    w_copies = [
        pltpu.make_async_copy(
            w_hbm.at[kt, kh], wv.at[kt, :, pl.ds(kh * C, C)], w_sem.at[kt * 3 + kh]
        )
        for kt in range(3)
        for kh in range(3)
    ]
    p_copies = [
        pltpu.make_async_copy(p, params.at[k, 0], p_sem.at[k])
        for k, p in enumerate((gain_hbm, nbias_hbm, cbias_hbm))
    ]
    barrier = pltpu.get_barrier_semaphore()
    for d in range(1, n):
        pl.semaphore_signal(barrier, inc=1, device_id=peer(d), device_id_type=MESH)
    for c in x_copies + p_copies:
        c.start()
    pl.semaphore_wait(barrier, n - 1)

    def row_of(i):
        return jnp.where(i == 0, 0, jnp.where(i == 1, H - 1, i - 1))

    def halo_copy(i, r):
        return pltpu.make_async_remote_copy(
            src_ref=x_hbm.at[pl.ds(F - 2, 2), pl.ds(r, 1)],
            dst_ref=hraw.at[:, pl.ds(r, 1)],
            send_sem=halo_send.at[i],
            recv_sem=halo_recv.at[i],
            device_id={"tm": lax.rem(tm + 1, T), "rows": row},
            device_id_type=MESH,
        )

    def own_edge(side):
        r = H - 1 if side == 0 else 0
        target = row + 1 if side == 0 else row - 1
        return pltpu.make_async_remote_copy(
            src_ref=x_hbm.at[:, pl.ds(r, 1)],
            dst_ref=eown.at[side],
            send_sem=eown_send.at[side],
            recv_sem=eown_recv.at[side],
            device_id={"tm": tm, "rows": lax.rem(target + R, R)},
            device_id_type=MESH,
        )

    def halo_edge(side):
        r = H - 1 if side == 0 else 0
        target = row + 1 if side == 0 else row - 1
        return pltpu.make_async_remote_copy(
            src_ref=hraw.at[:, pl.ds(r, 1)],
            dst_ref=ehalo.at[side],
            send_sem=ehalo_send.at[side],
            recv_sem=ehalo_recv.at[side],
            device_id={"tm": tm, "rows": lax.rem(target + R, R)},
            device_id_type=MESH,
        )

    has_next, has_prev = tm < T - 1, tm > 0
    sends_edge = (row < R - 1, row > 0)
    gets_edge = (row > 0, row < R - 1)

    @pl.when(has_next)
    def _():
        for i in range(EARLY):
            halo_copy(i, 0 if i == 0 else H - 1 if i == 1 else i - 1).start()

    for side in range(2):
        @pl.when(sends_edge[side])
        def _():
            own_edge(side).start()

    for c in w_copies:
        c.start()

    total = jnp.zeros((8, C), jnp.float32)
    square = jnp.zeros((8, C), jnp.float32)
    for f in range(F):
        x_copies[f].wait()

        def add_rows(r, carry):
            v = xv[f, r].astype(jnp.float32).reshape(W // 8, 8, C)
            return carry[0] + jnp.sum(v, axis=0), carry[1] + jnp.sum(v * v, axis=0)

        total, square = lax.fori_loop(0, H, add_rows, (total, square))
    stats[0, 0:8] = total
    stats[0, 8:16] = square

    def stat_copy(d):
        return pltpu.make_async_remote_copy(
            src_ref=stats.at[0],
            dst_ref=stats.at[d],
            send_sem=stat_send.at[d],
            recv_sem=stat_recv.at[d],
            device_id=peer(d),
            device_id_type=MESH,
        )

    for d in range(1, n):
        stat_copy(d).start()

    @pl.when(has_next)
    def _():
        for i in range(EARLY, H):
            halo_copy(i, 0 if i == 0 else H - 1 if i == 1 else i - 1).start()

    for c in p_copies:
        c.wait()
    for f in range(F):
        def start_acc(r, _):
            acc[f, r + 1] = xv[f, r].astype(jnp.float32) + params[2]
            return 0

        lax.fori_loop(0, H, start_acc, 0)
    for d in range(1, n):
        stat_copy(d).wait_recv()
    total = stats[0]
    for d in range(1, n):
        total = total + stats[d]
    sums = jnp.concatenate(
        [
            jnp.broadcast_to(jnp.sum(total[0:8], axis=0, keepdims=True), (8, C)),
            jnp.broadcast_to(jnp.sum(total[8:16], axis=0, keepdims=True), (8, C)),
        ],
        axis=0,
    )
    per_group = C // GROUPS
    channel = lax.broadcasted_iota(jnp.int32, (C, C), 0)
    other = lax.broadcasted_iota(jnp.int32, (C, C), 1)
    first = (other // per_group) * per_group
    member = jnp.where((channel >= first) & (channel < first + per_group), 1.0, 0.0)
    cells = 1.0 * F * H * W * per_group * n
    moments = (
        jnp.dot(
            sums,
            member.astype(jnp.float32),
            preferred_element_type=jnp.float32,
            precision=lax.Precision.HIGHEST,
        )
        / cells
    )
    mean = moments[0:1]
    var = jnp.maximum(moments[8:9] - mean * mean, 0.0)
    half_scale = lax.rsqrt(var + epsilon) * params[0] * 0.5
    half_bias = params[1] * 0.5

    column = lax.broadcasted_iota(jnp.int32, (W, C), 0)

    def activate(raw, put):
        h = (raw.astype(jnp.float32) - mean) * half_scale + half_bias
        a = h + h * jnp.tanh(h)
        put(0, jnp.where(column == 0, 0.0, pltpu.roll(a, 1, 0)).astype(jnp.bfloat16))
        put(1, a.astype(jnp.bfloat16))
        put(2, jnp.where(column == W - 1, 0.0, pltpu.roll(a, W - 1, 0)).astype(jnp.bfloat16))

    for f in range(F):
        def own_row(r, _):
            def put(k, v):
                own3[f, r, :, k * C : (k + 1) * C] = v

            activate(xv[f, r], put)
            return 0

        lax.fori_loop(0, H, own_row, 0)

    @pl.when(has_prev)
    def _():
        for i in range(2):
            halo_copy(i, 0 if i == 0 else H - 1).wait_recv()
        for side in range(2):
            @pl.when(sends_edge[side])
            def _():
                halo_edge(side).start()

    for c in w_copies:
        c.wait()

    def product(lhs, kt, lo=0, hi=3):
        return jnp.dot(
            lhs, wv[kt, :, lo * C : hi * C], preferred_element_type=jnp.float32
        )

    def finish(r, _):
        for f in range(F):
            out_ref[f, r] = acc[f, r + 1].astype(out_ref.dtype)
        return 0

    def own_rows(g, _):
        r0 = g * OWN_ROWS
        for kt in range(3):
            count = F - 2 + kt
            if count <= 0:
                continue
            lhs = own3[0:count, pl.ds(r0, OWN_ROWS)].reshape(count * OWN_ROWS * W, C3)
            y = product(lhs, kt)
            for kh in range(3):
                part = y[:, kh * C : (kh + 1) * C].reshape(count, OWN_ROWS, W, C)
                acc[2 - kt : 2 - kt + count, pl.ds(r0 + 2 - kh, OWN_ROWS)] += part
        return 0

    lax.fori_loop(0, H // OWN_ROWS, own_rows, 0)

    for side in range(2):
        kh = 0 if side == 0 else 2
        at = 1 if side == 0 else H

        @pl.when(gets_edge[side])
        def _():
            own_edge(side).wait_recv()
            for f in range(F):
                def put(k, v):
                    edge3[f, :, k * C : (k + 1) * C] = v

                activate(eown[side, f, 0], put)
            for kt in range(3):
                count = F - 2 + kt
                if count > 0:
                    lhs = edge3[0:count].reshape(count * W, C3)
                    acc[2 - kt : 2 - kt + count, at] += product(lhs, kt, kh, kh + 1).reshape(
                        count, W, C
                    )

    @pl.when(has_prev)
    def _():
        def halo_row(i, _):
            r = row_of(i)

            @pl.when(i >= 2)
            def _():
                halo_copy(i, r).wait_recv()

            for f in range(2):
                def put(k, v):
                    halo3[f, :, k * C : (k + 1) * C] = v

                activate(hraw[f, r], put)
            y = product(halo3[...].reshape(2 * W, C3), 0)
            z = product(halo3[1], 1)
            for kh in range(3):
                cols = slice(kh * C, (kh + 1) * C)
                acc[0, r + 2 - kh] += y[:W, cols] + z[:, cols]
                acc[1, r + 2 - kh] += y[W:, cols]

            @pl.when(i >= 2)
            def _():
                finish(i - 2, 0)

            return 0

        lax.fori_loop(0, 2, halo_row, 0)
        for side in range(2):
            kh = 0 if side == 0 else 2
            at = 1 if side == 0 else H

            @pl.when(gets_edge[side])
            def _():
                halo_edge(side).wait_recv()
                for f in range(2):
                    def put(k, v):
                        halo3[f, :, k * C : (k + 1) * C] = v

                    activate(ehalo[side, f, 0], put)
                y = product(halo3[...].reshape(2 * W, C3), 0, kh, kh + 1)
                z = product(halo3[1], 1, kh, kh + 1)
                acc[0, at] += y[:W] + z
                acc[1, at] += y[W:]

        lax.fori_loop(2, H, halo_row, 0)
        lax.fori_loop(max(H - 2, 0), H, finish, 0)

    @pl.when(jnp.logical_not(has_prev))
    def _():
        lax.fori_loop(0, H, finish, 0)

    for d in range(1, n):
        stat_copy(d).wait_send()

    @pl.when(has_next)
    def _():
        for i in range(H):
            halo_copy(i, 0 if i == 0 else H - 1 if i == 1 else i - 1).wait_send()

    for side in range(2):
        @pl.when(sends_edge[side])
        def _():
            own_edge(side).wait_send()

            @pl.when(has_prev)
            def _():
                halo_edge(side).wait_send()


def shards(T, R, inputs, norm_gain, norm_bias, conv_weight, conv_bias):
    _, F, H, W, C = inputs.shape
    n = T * R

    def pin(a):
        return pltpu.with_memory_space_constraint(a, pltpu.HBM)

    vmem = pl.BlockSpec(memory_space=pltpu.VMEM)
    hbm = pl.BlockSpec(memory_space=pltpu.HBM)
    anywhere = pl.BlockSpec(memory_space=pl.ANY)
    dma = pltpu.SemaphoreType.DMA
    out = pl.pallas_call(
        functools.partial(block_kernel, T, R),
        out_shape=jax.ShapeDtypeStruct((F, H, W, C), inputs.dtype),
        in_specs=[hbm, anywhere, anywhere, hbm, anywhere],
        out_specs=vmem,
        scratch_shapes=[
            pltpu.VMEM((3, 1, C), jnp.float32),
            dma((3,)),
            pltpu.VMEM((F, H, W, C), jnp.bfloat16),
            pltpu.VMEM((3, 3 * C, 3 * C), jnp.bfloat16),
            pltpu.VMEM((2, H, W, C), jnp.bfloat16),
            pltpu.VMEM((2, F, 1, W, C), jnp.bfloat16),
            pltpu.VMEM((2, 2, 1, W, C), jnp.bfloat16),
            pltpu.VMEM((F, H, W, 3 * C), jnp.bfloat16),
            pltpu.VMEM((2, W, 3 * C), jnp.bfloat16),
            pltpu.VMEM((F, W, 3 * C), jnp.bfloat16),
            pltpu.VMEM((F, H + 2, W, C), jnp.float32),
            pltpu.VMEM((n, 16, C), jnp.float32),
            dma((F,)),
            dma((9,)),
            dma((H,)),
            dma((H,)),
            dma((2,)),
            dma((2,)),
            dma((2,)),
            dma((2,)),
            dma((n,)),
            dma((n,)),
        ],
        compiler_params=pltpu.CompilerParams(
            collective_id=0, has_side_effects=True, vmem_limit_bytes=50 * 1024 * 1024
        ),
        name="norm_conv_block",
    )(
        pin(inputs.reshape(F, H, W, C)),
        pin(norm_gain),
        pin(norm_bias),
        pin(conv_weight.reshape(3, 3, 3 * C, C)),
        pin(conv_bias),
    )
    return out.reshape(inputs.shape)


def solution(mesh):
    placed = (P("batch", "tm", "rows", None, None), P(), P(), P(), P())
    return jax.shard_map(
        functools.partial(shards, mesh.shape["tm"], mesh.shape["rows"]),
        mesh=mesh,
        in_specs=placed,
        out_specs=P("batch", "tm", "rows", None, None),
        check_vma=False,
    )
```
